128 devices in a mesh: row: 8 (over z_hi, x), col: 16 (over z_lo, y, core).
Axes of the slice: x: 4, y: 4, z: 4 (z_hi: 2, z_lo: 2; z = z_hi * 2 + z_lo), core: 2. Of those that a mesh axis runs over, the one named last changes fastest.
Arguments:
- tokens: bfloat16 [16384, 2048], P(('row', 'col')), may hold values from -6 to 6
- expert_ids: int32 [16384, 8], P(('row', 'col')), may hold values from 0 to 127, all different within a row; in each aligned block of 128 rows (0 to 127, 128 to 255, ...) at most 10 rows name the same one
- gate_probs: float32 [16384, 8], P(('row', 'col')), may hold values from 0.05 to 0.5
- w_gate: bfloat16 [128, 2048, 768], P(('row', 'col')), may hold values from -0.125 to 0.125
- w_up: bfloat16 [128, 2048, 768], P(('row', 'col')), may hold values from -0.125 to 0.125
- w_down: bfloat16 [128, 768, 2048], P(('row', 'col')), may hold values from -0.21875 to 0.21875
Outputs:
- mixed: bfloat16 [16384, 2048], P(('row', 'col'))
The draws below stay inside these ranges and needn't reach their ends.
Inputs may be any that keep to these rules, and one draw needn't show every extreme that they name: `expert_ids`: each row names 8 different experts; among the rows of one device (aligned blocks of 128 rows) no expert is named more than 10 times.
All inputs are finite; a program needn't handle non-finite values.
Results may differ from the reference program's by a relative error of at most 0.0058.
Values may be sent and summed in bfloat16 or wider, within the bound.
No kernel may reach another device: no remote copies, remote signals or barrier semaphores. Data moves between devices by JAX's collectives and lax.ppermute only.
A program may use at most 128 MiB of HBM per device.

```python
import math
import jax
import jax.numpy as jnp
import numpy as np
from jax import lax

D = 2048
FF = 768
TOPK = 8
TOK_DEV = 128
EXPERTS = 128
TOKENS = 16384
SLOTS = 10
N_ROW = 8
N_COL = 16


def level_of(stream_key, extent, shards, smallest, high):
    def one(axis_at, blocks):
        draws = jax.random.uniform(jax.random.fold_in(jax.random.fold_in(stream_key, 6), axis_at), (blocks,), jnp.float32, smallest / len(shards), high / len(shards))
        return jnp.repeat(jnp.exp(draws), extent[axis_at] // blocks).reshape((-1,) + (1,) * (len(extent) - axis_at - 1))

    loudness = one(*shards[0])
    for cut in shards[1:]:
        loudness = loudness * one(*cut)
    return loudness


def shared_out(own_key, own, number, rows, count, top, most, slope):
    order = jax.random.permutation(own_key, count)
    crowded, ordinary = load_shares(count, rows * top, most, slope, True), load_shares(count, rows * top, most, slope, False)
    places = jnp.arange(count)

    def named(lengths, rotation):
        used = int((lengths > 0).sum())
        fixed = max(1, used // 4)
        shifted = fixed + (places - fixed + rotation * (used - fixed)) % max(1, count - fixed)
        return jnp.zeros((count,), jnp.int32).at[order[jnp.where(places < fixed, places, shifted)]].set(jnp.asarray(lengths, jnp.int32))

    lengths = jnp.where(number % 4 == 0, named(crowded, number // 4), named(ordinary, number - number // 4 - 1))
    mixed = jax.random.permutation(jax.random.fold_in(own, 3), count)
    source_of, taker = mixed[0:count // 2 * 2:2], mixed[1:count // 2 * 2:2]
    room = jnp.minimum(lengths[source_of] - 1, most - lengths[taker]) // 2
    room = jnp.where((source_of == order[0]) | (taker == order[0]) | (lengths[taker] == 0), 0, jnp.maximum(room, 0))
    shifted = jax.random.randint(jax.random.fold_in(own, 4), (count // 2,), 0, 1 << 20) % (room + 1)
    lengths = lengths.at[source_of].add(-shifted).at[taker].add(shifted)
    members = jnp.searchsorted(jnp.cumsum(lengths), jnp.arange(rows * top), side="right").astype(jnp.int32)
    listing = members.reshape(top, rows).T
    listing = listing[jax.random.permutation(jax.random.fold_in(own, 1), rows)]
    rotation = jax.random.randint(jax.random.fold_in(own, 2), (rows, 1), 0, top)
    return jnp.take_along_axis(listing, (jnp.arange(top)[None, :] + rotation) % top, axis=1)


def load_shares(number_of, total, most, slope, full):
    loads = [(1 << 20) // math.isqrt(rank ** slope) + 1 for rank in range(1, number_of + 1)]
    largest = most if full else min(most, max(-(-total // number_of), total * loads[0] // sum(loads)))
    least = 1 if total - largest >= number_of - 1 else 0
    counts, rest = [largest] + [least] * (number_of - 1), total - largest - least * (number_of - 1)
    while rest > 0:
        movable = [i for i in range(1, number_of) if counts[i] < largest] or [i for i in range(1, number_of) if counts[i] < most]
        whole, left = sum([loads[i] for i in movable]), rest
        for i in movable:
            addition = min(most - counts[i], max(1, left * loads[i] // whole), rest)
            counts[i] = counts[i] + addition
            rest = rest - addition
    return np.array(counts)


def gaussian(key, shape, deviation, bound, cuts=(), held_as=jnp.bfloat16):
    drawn = deviation * jax.random.normal(key, shape, jnp.float32)
    if cuts:
        drawn = drawn * level_of(key, shape, cuts, -0.22, 0.18)
    return jnp.clip(drawn, -bound, bound).astype(held_as)


def setup_inputs(seed: int = 0) -> dict:
    seeds = jax.random.split(jax.random.key(seed), 7)
    tokens = gaussian(seeds[0], (TOKENS, D), 1.0, 6.0, ((0, 128),))
    expert_ids_keys = jax.random.split(jax.random.fold_in(seeds[1], 1), TOKENS // TOK_DEV)
    expert_ids_turns = jax.random.permutation(jax.random.fold_in(seeds[1], 3), TOKENS // TOK_DEV)
    expert_ids = jax.vmap(lambda own, number: shared_out(jax.random.fold_in(seeds[1], 2), own, number, TOK_DEV, EXPERTS, TOPK, SLOTS, 2))(expert_ids_keys, expert_ids_turns).reshape((TOKENS, TOPK))
    gate_probs = jnp.clip(0.05 + 0.45 * jax.random.uniform(seeds[2], (TOKENS, TOPK), jnp.float32) ** level_of(seeds[2], (TOKENS, TOPK), ((0, 128),), -0.2, 0.2), 0.05, 0.5)
    w_gate = gaussian(seeds[3], (EXPERTS, D, FF), D ** -0.5, 0.125, ((0, 128),))
    w_up = gaussian(seeds[4], (EXPERTS, D, FF), D ** -0.5, 0.125, ((0, 128),))
    w_down = gaussian(seeds[5], (EXPERTS, FF, D), FF ** -0.5, 0.21875, ((0, 128),))
    return dict(tokens=tokens, expert_ids=expert_ids, gate_probs=gate_probs, w_gate=w_gate, w_up=w_up, w_down=w_down)


def reference(tokens, expert_ids, gate_probs, w_gate, w_up, w_down):
    sources = N_ROW * N_COL
    flat_ids = expert_ids.reshape(sources, TOK_DEV * TOPK)
    onehot = (flat_ids[:, :, None] == jnp.arange(EXPERTS, dtype=jnp.int32)[None, None, :]).astype(jnp.int32)
    rank = jnp.sum((jnp.cumsum(onehot, axis=1) - 1) * onehot, axis=2).astype(jnp.int32)
    source = jnp.arange(sources, dtype=jnp.int32)[:, None]
    position = (flat_ids * (sources * SLOTS) + source * SLOTS + rank).reshape(-1).astype(jnp.int32)
    token_of = (jnp.arange(TOKENS * TOPK, dtype=jnp.int32) // TOPK).astype(jnp.int32)
    owner = jnp.full((EXPERTS * sources * SLOTS,), -1, jnp.int32).at[position].set(token_of)
    owner = owner.reshape(EXPERTS, sources * SLOTS)

    def one_expert(index):
        picks = owner[index]
        rows = tokens[jnp.maximum(picks, 0)]
        rows = jnp.where((picks >= 0)[:, None], rows, jnp.zeros((), tokens.dtype))
        gate = jnp.dot(rows, w_gate[index], preferred_element_type=jnp.float32)
        up = jnp.dot(rows, w_up[index], preferred_element_type=jnp.float32)
        hidden = (jax.nn.silu(gate) * up).astype(jnp.bfloat16)
        return jnp.dot(hidden, w_down[index], preferred_element_type=jnp.float32).astype(jnp.bfloat16)

    outputs = lax.map(one_expert, jnp.arange(EXPERTS, dtype=jnp.int32))
    picked = outputs.reshape(-1, D)[position].reshape(TOKENS, TOPK, D).astype(jnp.float32)
    mixed = jnp.sum(gate_probs.astype(jnp.float32)[:, :, None] * picked, axis=1)
    return mixed.astype(jnp.bfloat16)
```

```python
import functools

import jax
import jax.numpy as jnp
from jax import lax
from jax.experimental import pallas as pl
from jax.experimental.pallas import tpu as pltpu
from jax.sharding import PartitionSpec as P

BF = jnp.bfloat16
F32 = jnp.float32
LANES = 128
SUB = 16


def swap_matrix():
    i = lax.broadcasted_iota(jnp.int32, (SUB * SUB, SUB * SUB), 0)
    j = lax.broadcasted_iota(jnp.int32, (SUB * SUB, SUB * SUB), 1)
    return (j == (i % SUB) * SUB + i // SUB).astype(F32).astype(BF)


def dispatch_kernel(slots, ids_ref, tok_ref, out_ref, pos_ref, tiles, pos_smem, sem):
    top, rows = ids_ref.shape
    experts = out_ref.shape[0] // slots
    ids = ids_ref[...]
    expert = lax.broadcasted_iota(jnp.int32, (experts, rows), 0)
    named = jnp.zeros((experts, rows), F32)
    for k in range(top):
        named += (ids[k : k + 1, :] == expert).astype(F32)
    before = lax.broadcasted_iota(jnp.int32, (rows, rows), 0)
    after = lax.broadcasted_iota(jnp.int32, (rows, rows), 1)
    earlier = (before < after).astype(F32).astype(BF)
    rank = jnp.dot(named.astype(BF), earlier, preferred_element_type=F32)
    slot = expert.astype(F32) * slots + rank
    for k in range(top):
        mine = jnp.where(ids[k : k + 1, :] == expert, slot, 0.0)
        pos_ref[k : k + 1, :] = jnp.sum(mine, axis=0, keepdims=True).astype(jnp.int32)
    copy = pltpu.make_async_copy(pos_ref, pos_smem, sem)
    copy.start()

    swap = swap_matrix()
    for b in range(rows // (2 * SUB)):
        halves = []
        for h in range(2):
            at = (2 * b + h) * SUB
            halves.append(
                jnp.concatenate(
                    [tok_ref[at : at + SUB, c * LANES : (c + 1) * LANES] for c in range(SUB)], axis=0
                )
            )
        moved = jnp.dot(swap, jnp.concatenate(halves, axis=1), preferred_element_type=F32).astype(BF)
        for h in range(2):
            at = (2 * b + h) * SUB
            tiles[at : at + SUB] = moved[:, h * LANES : (h + 1) * LANES].reshape(SUB, SUB, LANES)

    def clear(i, _):
        for j in range(slots):
            out_ref[i * slots + j] = jnp.zeros((SUB, LANES), BF)
        return 0

    lax.fori_loop(0, experts, clear, 0)
    copy.wait()

    def place(t, _):
        tile = tiles[t]
        for k in range(top):
            out_ref[pos_smem[k, t]] = tile
        return 0

    lax.fori_loop(0, rows, place, 0)


def ffn_kernel(x_ref, wg_ref, wu_ref, wd_ref, out_ref, rows_ref):
    swap = swap_matrix()
    rows = rows_ref.shape[0]
    for b in range(rows // (2 * SUB)):
        lo = x_ref[(2 * b) * 256 : (2 * b + 1) * 256, :]
        hi = x_ref[(2 * b + 1) * 256 : (2 * b + 2) * 256, :]
        moved = jnp.dot(swap, jnp.concatenate([lo, hi], axis=1), preferred_element_type=F32).astype(BF)
        for h in range(2):
            for c in range(SUB):
                rows_ref[(2 * b + h) * SUB : (2 * b + h + 1) * SUB, c * LANES : (c + 1) * LANES] = moved[
                    c * SUB : (c + 1) * SUB, h * LANES : (h + 1) * LANES
                ]
    x = rows_ref[...]
    gate = jnp.dot(x, wg_ref[...], preferred_element_type=F32)
    up = jnp.dot(x, wu_ref[...], preferred_element_type=F32)
    hidden = (gate / (1.0 + jnp.exp(-gate)) * up).astype(BF)
    rows_ref[...] = jnp.dot(hidden, wd_ref[...], preferred_element_type=F32).astype(BF)
    for b in range(rows // (2 * SUB)):
        halves = []
        for h in range(2):
            at = (2 * b + h) * SUB
            halves.append(
                jnp.concatenate(
                    [rows_ref[at : at + SUB, c * LANES : (c + 1) * LANES] for c in range(SUB)], axis=0
                )
            )
        moved = jnp.dot(swap, jnp.concatenate(halves, axis=1), preferred_element_type=F32).astype(BF)
        for h in range(2):
            out_ref[(2 * b + h) * 256 : (2 * b + h + 1) * 256, :] = moved[:, h * LANES : (h + 1) * LANES]


def combine_kernel(pos_ref, prob_ref, x_ref, out_ref, tiles):
    top, rows = pos_ref.shape

    def mix(t, _):
        total = jnp.zeros((SUB, LANES), F32)
        for k in range(top):
            total += prob_ref[k, t] * x_ref[pos_ref[k, t]].astype(F32)
        tiles[t] = total.astype(BF)
        return 0

    lax.fori_loop(0, rows, mix, 0)
    swap = swap_matrix()
    for b in range(rows // (2 * SUB)):
        halves = []
        for h in range(2):
            at = (2 * b + h) * SUB
            halves.append(tiles[at : at + SUB].reshape(SUB * SUB, LANES))
        moved = jnp.dot(swap, jnp.concatenate(halves, axis=1), preferred_element_type=F32).astype(BF)
        for h in range(2):
            at = (2 * b + h) * SUB
            for c in range(SUB):
                out_ref[at : at + SUB, c * LANES : (c + 1) * LANES] = moved[
                    c * SUB : (c + 1) * SUB, h * LANES : (h + 1) * LANES
                ]


def body(tokens, expert_ids, gate_probs, w_gate, w_up, w_down):
    rows, top = expert_ids.shape
    width = tokens.shape[1]
    hidden = w_gate.shape[2]
    experts = lax.axis_size("row") * lax.axis_size("col")
    slots = 5 * rows * top // (4 * experts)
    total = experts * slots
    vmem = pl.BlockSpec(memory_space=pltpu.VMEM)
    smem = pl.BlockSpec(memory_space=pltpu.SMEM)
    limit = pltpu.CompilerParams(vmem_limit_bytes=56 * 1024 * 1024)

    buffer, pos = pl.pallas_call(
        functools.partial(dispatch_kernel, slots),
        out_shape=(
            jax.ShapeDtypeStruct((total, SUB, LANES), BF),
            jax.ShapeDtypeStruct((top, rows), jnp.int32),
        ),
        in_specs=[vmem, vmem],
        out_specs=(vmem, vmem),
        scratch_shapes=[
            pltpu.VMEM((rows, SUB, LANES), BF),
            pltpu.SMEM((top, rows), jnp.int32),
            pltpu.SemaphoreType.DMA,
        ],
        compiler_params=limit,
        name="dispatch",
    )(expert_ids.T, tokens)

    wire = buffer.reshape(experts, slots * SUB, LANES)
    wire = lax.all_to_all(wire, ("row", "col"), split_axis=0, concat_axis=0, tiled=True)

    step = 256
    whole = lambda i: (0, 0)
    wire = pl.pallas_call(
        ffn_kernel,
        grid=(total // step,),
        out_shape=jax.ShapeDtypeStruct((total * SUB, LANES), BF),
        in_specs=[
            pl.BlockSpec((step * SUB, LANES), lambda i: (i, 0)),
            pl.BlockSpec((width, hidden), whole),
            pl.BlockSpec((width, hidden), whole),
            pl.BlockSpec((hidden, width), whole),
        ],
        out_specs=pl.BlockSpec((step * SUB, LANES), lambda i: (i, 0)),
        scratch_shapes=[pltpu.VMEM((step, width), BF)],
        compiler_params=limit,
        name="ffn",
    )(wire.reshape(total * SUB, LANES), w_gate[0], w_up[0], w_down[0])

    wire = wire.reshape(experts, slots * SUB, LANES)
    wire = lax.all_to_all(wire, ("row", "col"), split_axis=0, concat_axis=0, tiled=True)

    return pl.pallas_call(
        combine_kernel,
        out_shape=jax.ShapeDtypeStruct((rows, width), BF),
        in_specs=[smem, smem, vmem],
        out_specs=vmem,
        scratch_shapes=[pltpu.VMEM((rows, SUB, LANES), BF)],
        compiler_params=limit,
        name="combine",
    )(pos, gate_probs.T, wire.reshape(total, SUB, LANES))


def solution(mesh):
    in_specs = (
        P(("row", "col"), None),
        P(("row", "col"), None),
        P(("row", "col"), None),
        P(("row", "col"), None, None),
        P(("row", "col"), None, None),
        P(("row", "col"), None, None),
    )
    out_specs = P(("row", "col"), None)
    return jax.shard_map(body, mesh=mesh, in_specs=in_specs, out_specs=out_specs, check_vma=False)
```

```python
import functools

import jax
import jax.numpy as jnp
from jax import lax
from jax.experimental import pallas as pl
from jax.experimental.pallas import tpu as pltpu
from jax.sharding import PartitionSpec as P

BF = jnp.bfloat16
F32 = jnp.float32
LANES = 128
SUB = 16


def swap_matrix():
    i = lax.broadcasted_iota(jnp.int32, (SUB * SUB, SUB * SUB), 0)
    j = lax.broadcasted_iota(jnp.int32, (SUB * SUB, SUB * SUB), 1)
    return (j == (i % SUB) * SUB + i // SUB).astype(F32).astype(BF)


def dispatch_kernel(slots, ids_ref, tok_ref, out_ref, pos_ref, tiles, pos_smem, sem):
    top, rows = ids_ref.shape
    experts = out_ref.shape[0] // slots
    ids = ids_ref[...]
    expert = lax.broadcasted_iota(jnp.int32, (experts, rows), 0)
    named = jnp.zeros((experts, rows), F32)
    for k in range(top):
        named += (ids[k : k + 1, :] == expert).astype(F32)
    before = lax.broadcasted_iota(jnp.int32, (rows, rows), 0)
    after = lax.broadcasted_iota(jnp.int32, (rows, rows), 1)
    earlier = (before < after).astype(F32).astype(BF)
    rank = jnp.dot(named.astype(BF), earlier, preferred_element_type=F32)
    slot = expert.astype(F32) * slots + rank
    for k in range(top):
        mine = jnp.where(ids[k : k + 1, :] == expert, slot, 0.0)
        pos_ref[k : k + 1, :] = jnp.sum(mine, axis=0, keepdims=True).astype(jnp.int32)
    copy = pltpu.make_async_copy(pos_ref, pos_smem, sem)
    copy.start()

    swap = swap_matrix()
    for b in range(rows // (2 * SUB)):
        halves = []
        for h in range(2):
            at = (2 * b + h) * SUB
            halves.append(
                jnp.concatenate(
                    [tok_ref[at : at + SUB, c * LANES : (c + 1) * LANES] for c in range(SUB)], axis=0
                )
            )
        moved = jnp.dot(swap, jnp.concatenate(halves, axis=1), preferred_element_type=F32).astype(BF)
        for h in range(2):
            at = (2 * b + h) * SUB
            tiles[at : at + SUB] = moved[:, h * LANES : (h + 1) * LANES].reshape(SUB, SUB, LANES)

    def clear(i, _):
        for j in range(slots):
            out_ref[i * slots + j] = jnp.zeros((SUB, LANES), BF)
        return 0

    lax.fori_loop(0, experts, clear, 0)
    copy.wait()

    def place(t, _):
        tile = tiles[t]
        for k in range(top):
            out_ref[pos_smem[k, t]] = tile
        return 0

    lax.fori_loop(0, rows, place, 0)


def ffn_kernel(x_ref, wg_ref, wu_ref, wd_ref, out_ref, rows_ref):
    swap = swap_matrix()
    rows = rows_ref.shape[0]
    for b in range(rows // (2 * SUB)):
        lo = x_ref[(2 * b) * 256 : (2 * b + 1) * 256, :]
        hi = x_ref[(2 * b + 1) * 256 : (2 * b + 2) * 256, :]
        moved = jnp.dot(swap, jnp.concatenate([lo, hi], axis=1), preferred_element_type=F32).astype(BF)
        for h in range(2):
            for c in range(SUB):
                rows_ref[(2 * b + h) * SUB : (2 * b + h + 1) * SUB, c * LANES : (c + 1) * LANES] = moved[
                    c * SUB : (c + 1) * SUB, h * LANES : (h + 1) * LANES
                ]
    x = rows_ref[...]
    gate = jnp.dot(x, wg_ref[...], preferred_element_type=F32)
    up = jnp.dot(x, wu_ref[...], preferred_element_type=F32)
    hidden = (gate / (1.0 + jnp.exp(-gate)) * up).astype(BF)
    rows_ref[...] = jnp.dot(hidden, wd_ref[...], preferred_element_type=F32).astype(BF)
    for b in range(rows // (2 * SUB)):
        halves = []
        for h in range(2):
            at = (2 * b + h) * SUB
            halves.append(
                jnp.concatenate(
                    [rows_ref[at : at + SUB, c * LANES : (c + 1) * LANES] for c in range(SUB)], axis=0
                )
            )
        moved = jnp.dot(swap, jnp.concatenate(halves, axis=1), preferred_element_type=F32).astype(BF)
        for h in range(2):
            out_ref[(2 * b + h) * 256 : (2 * b + h + 1) * 256, :] = moved[:, h * LANES : (h + 1) * LANES]


def combine_kernel(pos_ref, prob_ref, x_ref, out_ref, tiles):
    top, rows = pos_ref.shape

    def mix(t, _):
        total = jnp.zeros((SUB, LANES), F32)
        for k in range(top):
            total += prob_ref[k, t] * x_ref[pos_ref[k, t]].astype(F32)
        tiles[t] = total.astype(BF)
        return 0

    lax.fori_loop(0, rows, mix, 0)
    swap = swap_matrix()
    for b in range(rows // (2 * SUB)):
        halves = []
        for h in range(2):
            at = (2 * b + h) * SUB
            halves.append(tiles[at : at + SUB].reshape(SUB * SUB, LANES))
        moved = jnp.dot(swap, jnp.concatenate(halves, axis=1), preferred_element_type=F32).astype(BF)
        for h in range(2):
            at = (2 * b + h) * SUB
            for c in range(SUB):
                out_ref[at : at + SUB, c * LANES : (c + 1) * LANES] = moved[
                    c * SUB : (c + 1) * SUB, h * LANES : (h + 1) * LANES
                ]


def body(tokens, expert_ids, gate_probs, w_gate, w_up, w_down):
    rows, top = expert_ids.shape
    width = tokens.shape[1]
    hidden = w_gate.shape[2]
    experts = lax.axis_size("row") * lax.axis_size("col")
    slots = 5 * rows * top // (4 * experts)
    total = experts * slots
    vmem = pl.BlockSpec(memory_space=pltpu.VMEM)
    smem = pl.BlockSpec(memory_space=pltpu.SMEM)
    limit = pltpu.CompilerParams(vmem_limit_bytes=32 * 1024 * 1024)

    buffer, pos = pl.pallas_call(
        functools.partial(dispatch_kernel, slots),
        out_shape=(
            jax.ShapeDtypeStruct((total, SUB, LANES), BF),
            jax.ShapeDtypeStruct((top, rows), jnp.int32),
        ),
        in_specs=[vmem, vmem],
        out_specs=(vmem, vmem),
        scratch_shapes=[
            pltpu.VMEM((rows, SUB, LANES), BF),
            pltpu.SMEM((top, rows), jnp.int32),
            pltpu.SemaphoreType.DMA,
        ],
        compiler_params=limit,
        name="dispatch",
    )(expert_ids.T, tokens)

    wire = buffer.reshape(experts, slots * SUB, LANES)
    wire = lax.all_to_all(wire, ("row", "col"), split_axis=0, concat_axis=0, tiled=True)

    step = 256
    whole = lambda i: (0, 0)
    wire = pl.pallas_call(
        ffn_kernel,
        grid=(total // step,),
        out_shape=jax.ShapeDtypeStruct((total * SUB, LANES), BF),
        in_specs=[
            pl.BlockSpec((step * SUB, LANES), lambda i: (i, 0)),
            pl.BlockSpec((width, hidden), whole),
            pl.BlockSpec((width, hidden), whole),
            pl.BlockSpec((hidden, width), whole),
        ],
        out_specs=pl.BlockSpec((step * SUB, LANES), lambda i: (i, 0)),
        scratch_shapes=[pltpu.VMEM((step, width), BF)],
        compiler_params=limit,
        name="ffn",
    )(wire.reshape(total * SUB, LANES), w_gate[0], w_up[0], w_down[0])

    wire = wire.reshape(experts, slots * SUB, LANES)
    wire = lax.all_to_all(wire, ("row", "col"), split_axis=0, concat_axis=0, tiled=True)

    return pl.pallas_call(
        combine_kernel,
        out_shape=jax.ShapeDtypeStruct((rows, width), BF),
        in_specs=[smem, smem, vmem],
        out_specs=vmem,
        scratch_shapes=[pltpu.VMEM((rows, SUB, LANES), BF)],
        compiler_params=limit,
        name="combine",
    )(pos, gate_probs.T, wire.reshape(total, SUB, LANES))


def solution(mesh):
    in_specs = (
        P(("row", "col"), None),
        P(("row", "col"), None),
        P(("row", "col"), None),
        P(("row", "col"), None, None),
        P(("row", "col"), None, None),
        P(("row", "col"), None, None),
    )
    out_specs = P(("row", "col"), None)
    return jax.shard_map(body, mesh=mesh, in_specs=in_specs, out_specs=out_specs, check_vma=False)
```

```python
import functools

import jax
import jax.numpy as jnp
from jax import lax
from jax.experimental import pallas as pl
from jax.experimental.pallas import tpu as pltpu
from jax.sharding import PartitionSpec as P

BF = jnp.bfloat16
F32 = jnp.float32
LANES = 128
SUB = 16


def swap_matrix():
    i = lax.broadcasted_iota(jnp.int32, (SUB * SUB, SUB * SUB), 0)
    j = lax.broadcasted_iota(jnp.int32, (SUB * SUB, SUB * SUB), 1)
    return (j == (i % SUB) * SUB + i // SUB).astype(F32).astype(BF)


def dispatch_kernel(slots, ids_hbm, tok_hbm, out_ref, pos_ref, ids_ref, tok_ref, tiles, pos_smem, sems):
    top, rows = ids_ref.shape
    experts = out_ref.shape[0] // slots
    get_ids = pltpu.make_async_copy(ids_hbm, ids_ref, sems.at[0])
    get_tok = pltpu.make_async_copy(tok_hbm, tok_ref, sems.at[1])
    get_ids.start()
    get_tok.start()

    def clear(i, _):
        for j in range(4 * slots):
            out_ref[i * (4 * slots) + j] = jnp.zeros((SUB, LANES), BF)
        return 0

    lax.fori_loop(0, experts // 4, clear, 0)
    get_ids.wait()
    ids = ids_ref[...]
    expert = lax.broadcasted_iota(jnp.int32, (experts, rows), 0)
    named = jnp.zeros((experts, rows), F32)
    for k in range(top):
        named += (ids[k : k + 1, :] == expert).astype(F32)
    before = lax.broadcasted_iota(jnp.int32, (rows, rows), 0)
    after = lax.broadcasted_iota(jnp.int32, (rows, rows), 1)
    earlier = (before < after).astype(F32).astype(BF)
    rank = jnp.dot(named.astype(BF), earlier, preferred_element_type=F32)
    slot = expert.astype(F32) * slots + rank
    for k in range(top):
        mine = jnp.where(ids[k : k + 1, :] == expert, slot, 0.0)
        pos_ref[k : k + 1, :] = jnp.sum(mine, axis=0, keepdims=True).astype(jnp.int32)
    to_smem = pltpu.make_async_copy(pos_ref, pos_smem, sems.at[2])
    to_smem.start()

    get_tok.wait()
    swap = swap_matrix()
    for b in range(rows // (2 * SUB)):
        halves = []
        for h in range(2):
            at = (2 * b + h) * SUB
            halves.append(
                jnp.concatenate(
                    [tok_ref[at : at + SUB, c * LANES : (c + 1) * LANES] for c in range(SUB)], axis=0
                )
            )
        moved = jnp.dot(swap, jnp.concatenate(halves, axis=1), preferred_element_type=F32).astype(BF)
        for h in range(2):
            at = (2 * b + h) * SUB
            tiles[at : at + SUB] = moved[:, h * LANES : (h + 1) * LANES].reshape(SUB, SUB, LANES)
    to_smem.wait()

    def place(i, _):
        for j in range(4):
            t = i * 4 + j
            tile = tiles[t]
            for k in range(top):
                out_ref[pos_smem[k, t]] = tile
        return 0

    lax.fori_loop(0, rows // 4, place, 0)


def ffn_kernel(step, x_ref, wg_ref, wu_ref, wd_ref, out_ref, rows_ref):
    swap = swap_matrix()
    rows = step

    def block(i, _):
        base = i * (rows * SUB)
        for b in range(rows // (2 * SUB)):
            lo = x_ref[pl.ds(base + (2 * b) * 256, 256), :]
            hi = x_ref[pl.ds(base + (2 * b + 1) * 256, 256), :]
            moved = jnp.dot(swap, jnp.concatenate([lo, hi], axis=1), preferred_element_type=F32).astype(BF)
            for h in range(2):
                for c in range(SUB):
                    rows_ref[(2 * b + h) * SUB : (2 * b + h + 1) * SUB, c * LANES : (c + 1) * LANES] = moved[
                        c * SUB : (c + 1) * SUB, h * LANES : (h + 1) * LANES
                    ]
        x = rows_ref[...]
        gate = jnp.dot(x, wg_ref[...], preferred_element_type=F32)
        up = jnp.dot(x, wu_ref[...], preferred_element_type=F32)
        hidden = (gate / (1.0 + jnp.exp(-gate)) * up).astype(BF)
        rows_ref[...] = jnp.dot(hidden, wd_ref[...], preferred_element_type=F32).astype(BF)
        for b in range(rows // (2 * SUB)):
            halves = []
            for h in range(2):
                at = (2 * b + h) * SUB
                halves.append(
                    jnp.concatenate(
                        [rows_ref[at : at + SUB, c * LANES : (c + 1) * LANES] for c in range(SUB)], axis=0
                    )
                )
            moved = jnp.dot(swap, jnp.concatenate(halves, axis=1), preferred_element_type=F32).astype(BF)
            for h in range(2):
                out_ref[pl.ds(base + (2 * b + h) * 256, 256), :] = moved[:, h * LANES : (h + 1) * LANES]
        return 0

    lax.fori_loop(0, x_ref.shape[0] // (rows * SUB), block, 0)


def combine_kernel(pos_ref, prob_ref, x_ref, out_hbm, tiles, out_ref, sems):
    top, rows = pos_ref.shape
    swap = swap_matrix()
    part = 2 * SUB
    copies = []
    for b in range(rows // part):

        def mix(i, _):
            for j in range(4):
                t = i * 4 + j
                total = prob_ref[0, b * part + t] * x_ref[pos_ref[0, b * part + t]].astype(F32)
                for k in range(1, top):
                    total += prob_ref[k, b * part + t] * x_ref[pos_ref[k, b * part + t]].astype(F32)
                tiles[t] = total.astype(BF)
            return 0

        lax.fori_loop(0, part // 4, mix, 0)
        halves = [tiles[h * SUB : (h + 1) * SUB].reshape(SUB * SUB, LANES) for h in range(2)]
        moved = jnp.dot(swap, jnp.concatenate(halves, axis=1), preferred_element_type=F32).astype(BF)
        for h in range(2):
            at = (2 * b + h) * SUB
            for c in range(SUB):
                out_ref[at : at + SUB, c * LANES : (c + 1) * LANES] = moved[
                    c * SUB : (c + 1) * SUB, h * LANES : (h + 1) * LANES
                ]
        put = pltpu.make_async_copy(
            out_ref.at[pl.ds(b * part, part), :], out_hbm.at[pl.ds(b * part, part), :], sems.at[b]
        )
        put.start()
        copies.append(put)
    for put in copies:
        put.wait()


def in_hbm(x):
    return pltpu.with_memory_space_constraint(x, pltpu.HBM)


def body(tokens, expert_ids, gate_probs, w_gate, w_up, w_down):
    rows, top = expert_ids.shape
    width = tokens.shape[1]
    hidden = w_gate.shape[2]
    experts = lax.axis_size("row") * lax.axis_size("col")
    slots = 5 * rows * top // (4 * experts)
    total = experts * slots
    vmem = pl.BlockSpec(memory_space=pltpu.VMEM)
    smem = pl.BlockSpec(memory_space=pltpu.SMEM)
    hbm = pl.BlockSpec(memory_space=pltpu.HBM)
    limit = pltpu.CompilerParams(vmem_limit_bytes=32 * 1024 * 1024)

    buffer, pos = pl.pallas_call(
        functools.partial(dispatch_kernel, slots),
        out_shape=(
            jax.ShapeDtypeStruct((total, SUB, LANES), BF),
            jax.ShapeDtypeStruct((top, rows), jnp.int32),
        ),
        in_specs=[hbm, hbm],
        out_specs=(vmem, vmem),
        scratch_shapes=[
            pltpu.VMEM((top, rows), jnp.int32),
            pltpu.VMEM((rows, width), BF),
            pltpu.VMEM((rows, SUB, LANES), BF),
            pltpu.SMEM((top, rows), jnp.int32),
            pltpu.SemaphoreType.DMA((3,)),
        ],
        compiler_params=limit,
        name="dispatch",
    )(in_hbm(expert_ids.T), in_hbm(tokens))

    wire = buffer.reshape(experts, slots * SUB, LANES)
    wire = lax.all_to_all(wire, ("row", "col"), split_axis=0, concat_axis=0, tiled=True)

    step = 640
    wire = pl.pallas_call(
        functools.partial(ffn_kernel, step),
        out_shape=jax.ShapeDtypeStruct((total * SUB, LANES), BF),
        in_specs=[vmem] * 4,
        out_specs=vmem,
        scratch_shapes=[pltpu.VMEM((step, width), BF)],
        compiler_params=limit,
        name="ffn",
    )(wire.reshape(total * SUB, LANES), w_gate[0], w_up[0], w_down[0])

    wire = wire.reshape(experts, slots * SUB, LANES)
    wire = lax.all_to_all(wire, ("row", "col"), split_axis=0, concat_axis=0, tiled=True)

    return pl.pallas_call(
        combine_kernel,
        out_shape=jax.ShapeDtypeStruct((rows, width), BF),
        in_specs=[smem, smem, vmem],
        out_specs=hbm,
        scratch_shapes=[
            pltpu.VMEM((2 * SUB, SUB, LANES), BF),
            pltpu.VMEM((rows, width), BF),
            pltpu.SemaphoreType.DMA((rows // (2 * SUB),)),
        ],
        compiler_params=limit,
        name="combine",
    )(pos, gate_probs.T, wire.reshape(total, SUB, LANES))


def solution(mesh):
    in_specs = (
        P(("row", "col"), None),
        P(("row", "col"), None),
        P(("row", "col"), None),
        P(("row", "col"), None, None),
        P(("row", "col"), None, None),
        P(("row", "col"), None, None),
    )
    out_specs = P(("row", "col"), None)
    return jax.shard_map(body, mesh=mesh, in_specs=in_specs, out_specs=out_specs, check_vma=False)
```

```python
import functools
import math

import jax
import jax.numpy as jnp
from jax import lax
from jax.experimental import pallas as pl
from jax.experimental.pallas import tpu as pltpu
from jax.sharding import PartitionSpec as P

BF = jnp.bfloat16
F32 = jnp.float32
LANES = 128
SUB = 16


def swap_matrix():
    i = lax.broadcasted_iota(jnp.int32, (SUB * SUB, SUB * SUB), 0)
    j = lax.broadcasted_iota(jnp.int32, (SUB * SUB, SUB * SUB), 1)
    return (j == (i % SUB) * SUB + i // SUB).astype(F32).astype(BF)


def dispatch_kernel(slots, ids_hbm, tok_hbm, out_ref, pos_ref, ids_ref, tok_ref, tiles, pos_smem, sems):
    top, rows = ids_ref.shape
    experts = out_ref.shape[0] // slots
    get_ids = pltpu.make_async_copy(ids_hbm, ids_ref, sems.at[0])
    get_tok = pltpu.make_async_copy(tok_hbm, tok_ref, sems.at[1])
    get_ids.start()
    get_tok.start()

    def clear(i, _):
        for j in range(4 * slots):
            out_ref[i * (4 * slots) + j] = jnp.zeros((SUB, LANES), BF)
        return 0

    lax.fori_loop(0, experts // 4, clear, 0)
    get_ids.wait()
    ids = ids_ref[...]
    expert = lax.broadcasted_iota(jnp.int32, (experts, rows), 0)
    named = jnp.zeros((experts, rows), F32)
    for k in range(top):
        named += (ids[k : k + 1, :] == expert).astype(F32)
    before = lax.broadcasted_iota(jnp.int32, (rows, rows), 0)
    after = lax.broadcasted_iota(jnp.int32, (rows, rows), 1)
    earlier = (before < after).astype(F32).astype(BF)
    rank = jnp.dot(named.astype(BF), earlier, preferred_element_type=F32)
    slot = group_position(expert).astype(F32) * slots + rank
    for k in range(top):
        mine = jnp.where(ids[k : k + 1, :] == expert, slot, 0.0)
        pos_ref[k : k + 1, :] = jnp.sum(mine, axis=0, keepdims=True).astype(jnp.int32)
    to_smem = pltpu.make_async_copy(pos_ref, pos_smem, sems.at[2])
    to_smem.start()

    get_tok.wait()
    swap = swap_matrix()
    for b in range(rows // (2 * SUB)):
        halves = []
        for h in range(2):
            at = (2 * b + h) * SUB
            halves.append(
                jnp.concatenate(
                    [tok_ref[at : at + SUB, c * LANES : (c + 1) * LANES] for c in range(SUB)], axis=0
                )
            )
        moved = jnp.dot(swap, jnp.concatenate(halves, axis=1), preferred_element_type=F32).astype(BF)
        for h in range(2):
            at = (2 * b + h) * SUB
            tiles[at : at + SUB] = moved[:, h * LANES : (h + 1) * LANES].reshape(SUB, SUB, LANES)
    to_smem.wait()

    def place(i, _):
        for j in range(4):
            t = i * 4 + j
            tile = tiles[t]
            for k in range(top):
                out_ref[pos_smem[k, t]] = tile
        return 0

    lax.fori_loop(0, rows // 4, place, 0)


def ffn_kernel(step, x_ref, wg_ref, wu_ref, wd_ref, out_ref, rows_ref):
    swap = swap_matrix()
    rows = step

    def block(i, _):
        base = i * (rows * SUB)
        for b in range(rows // (2 * SUB)):
            lo = x_ref[pl.ds(base + (2 * b) * 256, 256), :]
            hi = x_ref[pl.ds(base + (2 * b + 1) * 256, 256), :]
            moved = jnp.dot(swap, jnp.concatenate([lo, hi], axis=1), preferred_element_type=F32).astype(BF)
            for h in range(2):
                for c in range(SUB):
                    rows_ref[(2 * b + h) * SUB : (2 * b + h + 1) * SUB, c * LANES : (c + 1) * LANES] = moved[
                        c * SUB : (c + 1) * SUB, h * LANES : (h + 1) * LANES
                    ]
        x = rows_ref[...]
        gate = jnp.dot(x, wg_ref[...], preferred_element_type=F32)
        up = jnp.dot(x, wu_ref[...], preferred_element_type=F32)
        hidden = (gate / (1.0 + jnp.exp(-gate)) * up).astype(BF)
        rows_ref[...] = jnp.dot(hidden, wd_ref[...], preferred_element_type=F32).astype(BF)
        for b in range(rows // (2 * SUB)):
            halves = []
            for h in range(2):
                at = (2 * b + h) * SUB
                halves.append(
                    jnp.concatenate(
                        [rows_ref[at : at + SUB, c * LANES : (c + 1) * LANES] for c in range(SUB)], axis=0
                    )
                )
            moved = jnp.dot(swap, jnp.concatenate(halves, axis=1), preferred_element_type=F32).astype(BF)
            for h in range(2):
                out_ref[pl.ds(base + (2 * b + h) * 256, 256), :] = moved[:, h * LANES : (h + 1) * LANES]
        return 0

    lax.fori_loop(0, x_ref.shape[0] // (rows * SUB), block, 0)


def combine_kernel(pos_ref, prob_ref, x_ref, out_hbm, tiles, out_ref, sems):
    top, rows = pos_ref.shape
    swap = swap_matrix()
    part = 2 * SUB
    copies = []
    for b in range(rows // part):

        def mix(i, _):
            for j in range(4):
                t = i * 4 + j
                total = prob_ref[0, b * part + t] * x_ref[pos_ref[0, b * part + t]].astype(F32)
                for k in range(1, top):
                    total += prob_ref[k, b * part + t] * x_ref[pos_ref[k, b * part + t]].astype(F32)
                tiles[t] = total.astype(BF)
            return 0

        lax.fori_loop(0, part // 4, mix, 0)
        halves = [tiles[h * SUB : (h + 1) * SUB].reshape(SUB * SUB, LANES) for h in range(2)]
        moved = jnp.dot(swap, jnp.concatenate(halves, axis=1), preferred_element_type=F32).astype(BF)
        for h in range(2):
            at = (2 * b + h) * SUB
            for c in range(SUB):
                out_ref[at : at + SUB, c * LANES : (c + 1) * LANES] = moved[
                    c * SUB : (c + 1) * SUB, h * LANES : (h + 1) * LANES
                ]
        put = pltpu.make_async_copy(
            out_ref.at[pl.ds(b * part, part), :], out_hbm.at[pl.ds(b * part, part), :], sems.at[b]
        )
        put.start()
        copies.append(put)
    for put in copies:
        put.wait()


AXES = (("zh", 2), ("x", 4), ("zl", 2), ("y", 4), ("core", 2))
ORDER = ("zh", "zl", "core", "x", "y")


def group_position(expert):
    digit, rest = {}, expert
    for name, size in reversed(AXES):
        digit[name], rest = rest % size, rest // size
    place = jnp.zeros_like(expert)
    for name in ORDER:
        place = place * dict(AXES)[name] + digit[name]
    return place


def in_hbm(x):
    return pltpu.with_memory_space_constraint(x, pltpu.HBM)


def body(tokens, expert_ids, gate_probs, w_gate, w_up, w_down):
    rows, top = expert_ids.shape
    width = tokens.shape[1]
    hidden = w_gate.shape[2]
    experts = math.prod(size for _, size in AXES)
    slots = 5 * rows * top // (4 * experts)
    total = experts * slots
    vmem = pl.BlockSpec(memory_space=pltpu.VMEM)
    smem = pl.BlockSpec(memory_space=pltpu.SMEM)
    hbm = pl.BlockSpec(memory_space=pltpu.HBM)
    limit = pltpu.CompilerParams(vmem_limit_bytes=32 * 1024 * 1024)

    buffer, pos = pl.pallas_call(
        functools.partial(dispatch_kernel, slots),
        out_shape=(
            jax.ShapeDtypeStruct((total, SUB, LANES), BF),
            jax.ShapeDtypeStruct((top, rows), jnp.int32),
        ),
        in_specs=[hbm, hbm],
        out_specs=(vmem, vmem),
        scratch_shapes=[
            pltpu.VMEM((top, rows), jnp.int32),
            pltpu.VMEM((rows, width), BF),
            pltpu.VMEM((rows, SUB, LANES), BF),
            pltpu.SMEM((top, rows), jnp.int32),
            pltpu.SemaphoreType.DMA((3,)),
        ],
        compiler_params=limit,
        name="dispatch",
    )(in_hbm(expert_ids.T), in_hbm(tokens))

    wire = buffer.reshape(experts, slots * SUB, LANES)
    wire = lax.all_to_all(wire, ORDER, split_axis=0, concat_axis=0, tiled=True)

    step = 640
    wire = pl.pallas_call(
        functools.partial(ffn_kernel, step),
        out_shape=jax.ShapeDtypeStruct((total * SUB, LANES), BF),
        in_specs=[vmem] * 4,
        out_specs=vmem,
        scratch_shapes=[pltpu.VMEM((step, width), BF)],
        compiler_params=limit,
        name="ffn",
    )(wire.reshape(total * SUB, LANES), w_gate[0], w_up[0], w_down[0])

    wire = wire.reshape(experts, slots * SUB, LANES)
    wire = lax.all_to_all(wire, ORDER, split_axis=0, concat_axis=0, tiled=True)

    return pl.pallas_call(
        combine_kernel,
        out_shape=jax.ShapeDtypeStruct((rows, width), BF),
        in_specs=[smem, smem, vmem],
        out_specs=hbm,
        scratch_shapes=[
            pltpu.VMEM((2 * SUB, SUB, LANES), BF),
            pltpu.VMEM((rows, width), BF),
            pltpu.SemaphoreType.DMA((rows // (2 * SUB),)),
        ],
        compiler_params=limit,
        name="combine",
    )(pos, gate_probs.T, wire.reshape(total, SUB, LANES))


def solution(mesh):
    names, sizes = zip(*AXES)
    fine = jax.sharding.Mesh(mesh.devices.reshape(sizes), names)
    return jax.shard_map(
        body,
        mesh=fine,
        in_specs=(P(names, None),) * 3 + (P(names, None, None),) * 3,
        out_specs=P(names, None),
        check_vma=False,
    )
```

```python
import functools
import math

import jax
import jax.numpy as jnp
from jax import lax
from jax.experimental import pallas as pl
from jax.experimental.pallas import tpu as pltpu
from jax.sharding import PartitionSpec as P

BF = jnp.bfloat16
F32 = jnp.float32
LANES = 128
SUB = 16


def swap_matrix():
    i = lax.broadcasted_iota(jnp.int32, (SUB * SUB, SUB * SUB), 0)
    j = lax.broadcasted_iota(jnp.int32, (SUB * SUB, SUB * SUB), 1)
    return (j == (i % SUB) * SUB + i // SUB).astype(F32).astype(BF)


def dispatch_kernel(
    slots, ids_hbm, prob_hbm, tok_hbm, out_ref, mix_ref, ids_ref, prob_ref, pos_ref, tok_ref, tiles, pos_smem, sems
):
    top, rows = ids_ref.shape
    experts = out_ref.shape[0] // slots
    get_ids = pltpu.make_async_copy(ids_hbm, ids_ref, sems.at[0])
    get_tok = pltpu.make_async_copy(tok_hbm, tok_ref, sems.at[1])
    get_prob = pltpu.make_async_copy(prob_hbm, prob_ref, sems.at[3])
    get_ids.start()
    get_prob.start()
    get_tok.start()

    def clear(i, _):
        for j in range(4 * slots):
            out_ref[i * (4 * slots) + j] = jnp.zeros((SUB, LANES), BF)
        return 0

    lax.fori_loop(0, experts // 4, clear, 0)
    get_ids.wait()
    ids = group_position(ids_ref[...])
    expert = lax.broadcasted_iota(jnp.int32, (experts, rows), 0)
    named = jnp.zeros((experts, rows), F32)
    for k in range(top):
        named += (ids[k : k + 1, :] == expert).astype(F32)
    before = lax.broadcasted_iota(jnp.int32, (rows, rows), 0)
    after = lax.broadcasted_iota(jnp.int32, (rows, rows), 1)
    earlier = (before < after).astype(F32).astype(BF)
    rank = jnp.dot(named.astype(BF), earlier, preferred_element_type=F32)
    slot = expert.astype(F32) * slots + rank
    for k in range(top):
        mine = jnp.where(ids[k : k + 1, :] == expert, slot, 0.0)
        pos_ref[k : k + 1, :] = jnp.sum(mine, axis=0, keepdims=True).astype(jnp.int32)
    to_smem = pltpu.make_async_copy(pos_ref, pos_smem, sems.at[2])
    to_smem.start()
    get_prob.wait()
    weigh(slots, ids, prob_ref[...], named, rank, mix_ref)

    get_tok.wait()
    swap = swap_matrix()
    for b in range(rows // (2 * SUB)):
        halves = []
        for h in range(2):
            at = (2 * b + h) * SUB
            halves.append(
                jnp.concatenate(
                    [tok_ref[at : at + SUB, c * LANES : (c + 1) * LANES] for c in range(SUB)], axis=0
                )
            )
        moved = jnp.dot(swap, jnp.concatenate(halves, axis=1), preferred_element_type=F32).astype(BF)
        for h in range(2):
            at = (2 * b + h) * SUB
            tiles[at : at + SUB] = moved[:, h * LANES : (h + 1) * LANES].reshape(SUB, SUB, LANES)
    to_smem.wait()

    def place(i, _):
        for j in range(4):
            t = i * 4 + j
            tile = tiles[t]
            for k in range(top):
                out_ref[pos_smem[k, t]] = tile
        return 0

    lax.fori_loop(0, rows // 4, place, 0)


def pair_matrix(to_pairs):
    i = lax.broadcasted_iota(jnp.int32, (256, 256), 0)
    j = lax.broadcasted_iota(jnp.int32, (256, 256), 1)
    if to_pairs:
        source = (i // 2 % SUB) * 16 + (i // 32) * 2 + i % 2
    else:
        source = (i // 2 % 8) * 32 + (i // 16) * 2 + i % 2
    return (j == source).astype(F32).astype(BF)


def ffn_kernel(slots, x_ref, wg_ref, wu_ref, wd_ref, out_ref, rows_ref, tail_ref):
    swap = swap_matrix()
    sources = out_ref.shape[0]
    chunk = slots * SUB
    main = 8 * sources
    groups = []
    for g in range(sources // 2):
        groups.append([(2 * g + h) * chunk for h in range(2)])
    for g in range(sources // 8):
        groups.append([(8 * g + h) * chunk + 8 * SUB for h in range(8)])
    for b in range(len(groups) // 2):
        halves = []
        for h in range(2):
            starts = groups[2 * b + h]
            size = 256 // len(starts)
            halves.append(jnp.concatenate([x_ref[at : at + size, :] for at in starts], axis=0))
        moved = jnp.dot(swap, jnp.concatenate(halves, axis=1), preferred_element_type=F32).astype(BF)
        for h in range(2):
            for c in range(SUB):
                rows_ref[(2 * b + h) * SUB : (2 * b + h + 1) * SUB, c * LANES : (c + 1) * LANES] = moved[
                    c * SUB : (c + 1) * SUB, h * LANES : (h + 1) * LANES
                ]
    x = rows_ref[...]
    gate = jnp.dot(x, wg_ref[...], preferred_element_type=F32)
    up = jnp.dot(x, wu_ref[...], preferred_element_type=F32)
    hidden = (gate / (1.0 + jnp.exp(-gate)) * up).astype(BF)
    for n in range(SUB // 2):
        cols = slice(n * 256, (n + 1) * 256)
        result = jnp.dot(hidden, wd_ref[:, cols], preferred_element_type=F32).astype(BF)
        for h in range(2):
            half = result[:, h * LANES : (h + 1) * LANES]
            out_ref[:, 2 * n + h] = half[:main].reshape(sources, 8, LANES)
        tail_ref[:, cols] = result[main:]
    pairs = pair_matrix(True)
    for b in range(sources // 16):
        halves = []
        for h in range(2):
            at = (2 * b + h) * SUB
            halves.append(
                jnp.concatenate(
                    [tail_ref[at : at + SUB, c * LANES : (c + 1) * LANES] for c in range(SUB)], axis=0
                )
            )
        moved = jnp.dot(pairs, jnp.concatenate(halves, axis=1), preferred_element_type=F32).astype(BF)
        for h in range(2):
            at = (2 * b + h) * 8
            out_ref[at : at + 8, SUB : 2 * slots] = moved[:, h * LANES : (h + 1) * LANES].reshape(
                8, 2 * slots - SUB, 8, LANES
            )


def weigh(slots, place, prob, named, rank, out_ref):
    top, rows = place.shape
    total = out_ref.shape[1]
    experts = total // slots
    expert = lax.broadcasted_iota(jnp.int32, (experts, rows), 0)
    weight = jnp.zeros((experts, rows), F32)
    for k in range(top):
        weight += jnp.where(place[k : k + 1, :] == expert, prob[k : k + 1, :], 0.0)
    rank = jnp.where(named > 0.0, rank, -1.0).T.astype(BF)
    weight = weight.T
    high = weight.astype(BF)
    low = (weight - high.astype(F32)).astype(BF)
    col = lax.broadcasted_iota(jnp.int32, (experts, total), 1)
    main = 8 * experts
    owner = jnp.where(col < main, col // 8, (col - main) // (slots - 8))
    spread = (owner == lax.broadcasted_iota(jnp.int32, (experts, total), 0)).astype(F32).astype(BF)
    col = lax.broadcasted_iota(jnp.int32, (rows, total), 1)
    slot = jnp.where(col < main, col % 8, 8 + (col - main) % (slots - 8)).astype(F32)
    mine = jnp.dot(rank, spread, preferred_element_type=F32) == slot
    for i, part in enumerate((high, low)):
        wide = jnp.dot(part, spread, preferred_element_type=F32)
        out_ref[i * rows : (i + 1) * rows, :] = jnp.where(mine, wide, 0.0).astype(BF)


def combine_kernel(slots, mix_ref, x_ref, out_hbm, tail_ref, out_ref, sems):
    experts = x_ref.shape[0]
    rows = out_ref.shape[0]
    main = 8 * experts
    pairs = pair_matrix(False)
    for b in range(experts // 16):
        halves = []
        for h in range(2):
            at = (2 * b + h) * 8
            halves.append(x_ref[at : at + 8, SUB : 2 * slots].reshape(256, LANES))
        moved = jnp.dot(pairs, jnp.concatenate(halves, axis=1), preferred_element_type=F32).astype(BF)
        for h in range(2):
            at = (2 * b + h) * SUB
            for c in range(SUB):
                tail_ref[at : at + SUB, c * LANES : (c + 1) * LANES] = moved[
                    c * SUB : (c + 1) * SUB, h * LANES : (h + 1) * LANES
                ]
    copies = []
    for n in range(SUB // 2):
        cols = slice(n * 256, (n + 1) * 256)
        block = jnp.concatenate([x_ref[:, 2 * n + h].reshape(main, LANES) for h in range(2)], axis=1)
        mixed = jnp.dot(mix_ref[:, :main], block, preferred_element_type=F32)
        mixed += jnp.dot(mix_ref[:, main:], tail_ref[:, cols], preferred_element_type=F32)
        out_ref[:, cols] = (mixed[:rows] + mixed[rows:]).astype(BF)
        if n % 4 == 3:
            part = pl.ds((n // 4) * 1024, 1024)
            put = pltpu.make_async_copy(out_ref.at[:, part], out_hbm.at[:, part], sems.at[n // 4])
            put.start()
            copies.append(put)
    for put in copies:
        put.wait()


AXES = (("zh", 2), ("x", 4), ("zl", 2), ("y", 4), ("core", 2))
ORDER = ("zh", "zl", "core", "x", "y")


def group_position(expert):
    digit, rest = {}, expert
    for name, size in reversed(AXES):
        digit[name], rest = rest % size, rest // size
    place = jnp.zeros_like(expert)
    for name in ORDER:
        place = place * dict(AXES)[name] + digit[name]
    return place


def in_hbm(x):
    return pltpu.with_memory_space_constraint(x, pltpu.HBM)


def body(tokens, expert_ids, gate_probs, w_gate, w_up, w_down):
    rows, top = expert_ids.shape
    width = tokens.shape[1]
    hidden = w_gate.shape[2]
    experts = math.prod(size for _, size in AXES)
    slots = 5 * rows * top // (4 * experts)
    total = experts * slots
    vmem = pl.BlockSpec(memory_space=pltpu.VMEM)
    hbm = pl.BlockSpec(memory_space=pltpu.HBM)
    limit = pltpu.CompilerParams(vmem_limit_bytes=32 * 1024 * 1024)

    buffer, mix = pl.pallas_call(
        functools.partial(dispatch_kernel, slots),
        out_shape=(
            jax.ShapeDtypeStruct((total, SUB, LANES), BF),
            jax.ShapeDtypeStruct((2 * rows, total), BF),
        ),
        in_specs=[hbm, hbm, hbm],
        out_specs=(vmem, vmem),
        scratch_shapes=[
            pltpu.VMEM((top, rows), jnp.int32),
            pltpu.VMEM((top, rows), F32),
            pltpu.VMEM((top, rows), jnp.int32),
            pltpu.VMEM((rows, width), BF),
            pltpu.VMEM((rows, SUB, LANES), BF),
            pltpu.SMEM((top, rows), jnp.int32),
            pltpu.SemaphoreType.DMA((4,)),
        ],
        compiler_params=limit,
        name="dispatch",
    )(in_hbm(expert_ids.T), in_hbm(gate_probs.T), in_hbm(tokens))

    wire = buffer.reshape(experts, slots * SUB, LANES)
    wire = lax.all_to_all(wire, ORDER, split_axis=0, concat_axis=0, tiled=True)

    wire = pl.pallas_call(
        functools.partial(ffn_kernel, slots),
        out_shape=jax.ShapeDtypeStruct((experts, 2 * slots, 8, LANES), BF),
        in_specs=[vmem] * 4,
        out_specs=vmem,
        scratch_shapes=[pltpu.VMEM((total, width), BF), pltpu.VMEM((total - 8 * experts, width), BF)],
        compiler_params=limit,
        name="ffn",
    )(wire.reshape(total * SUB, LANES), w_gate[0], w_up[0], w_down[0])

    wire = wire.reshape(experts, slots * SUB, LANES)
    wire = lax.all_to_all(wire, ORDER, split_axis=0, concat_axis=0, tiled=True)

    return pl.pallas_call(
        functools.partial(combine_kernel, slots),
        out_shape=jax.ShapeDtypeStruct((rows, width), BF),
        in_specs=[vmem, vmem],
        out_specs=hbm,
        scratch_shapes=[
            pltpu.VMEM((total - 8 * experts, width), BF),
            pltpu.VMEM((rows, width), BF),
            pltpu.SemaphoreType.DMA((2,)),
        ],
        compiler_params=limit,
        name="combine",
    )(mix, wire.reshape(experts, 2 * slots, 8, LANES))


def solution(mesh):
    names, sizes = zip(*AXES)
    fine = jax.sharding.Mesh(mesh.devices.reshape(sizes), names)
    return jax.shard_map(
        body,
        mesh=fine,
        in_specs=(P(names, None),) * 3 + (P(names, None, None),) * 3,
        out_specs=P(names, None),
        check_vma=False,
    )
```

```python
import functools
import math

import jax
import jax.numpy as jnp
from jax import lax
from jax.experimental import pallas as pl
from jax.experimental.pallas import tpu as pltpu
from jax.sharding import PartitionSpec as P

BF = jnp.bfloat16
F32 = jnp.float32
LANES = 128
SUB = 16


def pair_matrix(to_pairs):
    i = lax.broadcasted_iota(jnp.int32, (256, 256), 0)
    j = lax.broadcasted_iota(jnp.int32, (256, 256), 1)
    if to_pairs:
        source = (i // 2 % SUB) * 16 + (i // 32) * 2 + i % 2
    else:
        source = (i // 2 % 8) * 32 + (i // 16) * 2 + i % 2
    return (j == source).astype(F32).astype(BF)


def store_pairs(tail_ref, chunks):
    peers, tiles = chunks.shape[:2]
    pairs = pair_matrix(True)
    for b in range(peers // 16):
        halves = []
        for h in range(2):
            at = (2 * b + h) * SUB
            halves.append(
                jnp.concatenate(
                    [tail_ref[at : at + SUB, c * LANES : (c + 1) * LANES] for c in range(SUB)], axis=0
                )
            )
        moved = jnp.dot(pairs, jnp.concatenate(halves, axis=1), preferred_element_type=F32).astype(BF)
        for h in range(2):
            at = (2 * b + h) * 8
            chunks[at : at + 8, SUB:tiles] = moved[:, h * LANES : (h + 1) * LANES].reshape(8, tiles - SUB, 8, LANES)


def load_pairs(chunks, tail_ref):
    peers, tiles = chunks.shape[:2]
    pairs = pair_matrix(False)
    for b in range(peers // 16):
        halves = []
        for h in range(2):
            at = (2 * b + h) * 8
            halves.append(chunks[at : at + 8, SUB:tiles].reshape(256, LANES))
        moved = jnp.dot(pairs, jnp.concatenate(halves, axis=1), preferred_element_type=F32).astype(BF)
        for h in range(2):
            at = (2 * b + h) * SUB
            for c in range(SUB):
                tail_ref[at : at + SUB, c * LANES : (c + 1) * LANES] = moved[
                    c * SUB : (c + 1) * SUB, h * LANES : (h + 1) * LANES
                ]


def store_columns(result, n, chunks, tail_ref):
    peers = chunks.shape[0]
    main = 8 * peers
    for h in range(2):
        half = result[:, h * LANES : (h + 1) * LANES]
        chunks[:, 2 * n + h] = half[:main].reshape(peers, 8, LANES)
    tail_ref[:, n * 256 : (n + 1) * 256] = result[main:]


def columns_of(chunks, n):
    main = 8 * chunks.shape[0]
    return jnp.concatenate([chunks[:, 2 * n + h].reshape(main, LANES) for h in range(2)], axis=1)


def owner_and_slot(index, slots, experts):
    main = 8 * experts
    owner = jnp.where(index < main, index // 8, (index - main) // (slots - 8))
    slot = jnp.where(index < main, index % 8, 8 + (index - main) % (slots - 8))
    return owner, slot


def dispatch_kernel(slots, ids_hbm, prob_hbm, tok_hbm, out_ref, mix_ref, ids_ref, prob_ref, tok_ref, tail_ref, sems):
    top, rows = ids_ref.shape
    experts = out_ref.shape[0]
    total = experts * slots
    get_ids = pltpu.make_async_copy(ids_hbm, ids_ref, sems.at[0])
    get_prob = pltpu.make_async_copy(prob_hbm, prob_ref, sems.at[1])
    get_tok = pltpu.make_async_copy(tok_hbm, tok_ref, sems.at[2])
    get_ids.start()
    get_prob.start()
    get_tok.start()

    before = lax.broadcasted_iota(jnp.int32, (rows, rows), 0)
    after = lax.broadcasted_iota(jnp.int32, (rows, rows), 1)
    earlier = (before < after).astype(F32).astype(BF)
    owner, slot = owner_and_slot(lax.broadcasted_iota(jnp.int32, (total, experts), 0), slots, experts)
    from_expert = (owner == lax.broadcasted_iota(jnp.int32, (total, experts), 1)).astype(F32).astype(BF)
    get_ids.wait()
    get_prob.wait()
    place = group_position(ids_ref[...])
    prob = prob_ref[...]
    expert = lax.broadcasted_iota(jnp.int32, (experts, rows), 0)
    named = jnp.zeros((experts, rows), F32)
    weight = jnp.zeros((experts, rows), F32)
    for k in range(top):
        mine = place[k : k + 1, :] == expert
        named += mine.astype(F32)
        weight += jnp.where(mine, prob[k : k + 1, :], 0.0)
    rank = jnp.dot(named.astype(BF), earlier, preferred_element_type=F32)
    rank = jnp.where(named > 0.0, rank, -1.0)
    ranks = jnp.dot(from_expert, rank.astype(BF), preferred_element_type=F32)
    picked = (ranks == slot.astype(F32)).astype(F32).astype(BF)
    get_tok.wait()
    for n in range(SUB // 2):
        cols = slice(n * 256, (n + 1) * 256)
        store_columns(jnp.dot(picked, tok_ref[:, cols], preferred_element_type=F32).astype(BF), n, out_ref, tail_ref)
    store_pairs(tail_ref, out_ref)

    rank = rank.T.astype(BF)
    weight = weight.T
    high = weight.astype(BF)
    low = (weight - high.astype(F32)).astype(BF)
    owner, _ = owner_and_slot(lax.broadcasted_iota(jnp.int32, (experts, total), 1), slots, experts)
    _, slot = owner_and_slot(lax.broadcasted_iota(jnp.int32, (rows, total), 1), slots, experts)
    to_slot = (owner == lax.broadcasted_iota(jnp.int32, (experts, total), 0)).astype(F32).astype(BF)
    mine = jnp.dot(rank, to_slot, preferred_element_type=F32) == slot.astype(F32)
    for i, part in enumerate((high, low)):
        wide = jnp.dot(part, to_slot, preferred_element_type=F32)
        mix_ref[i * rows : (i + 1) * rows, :] = jnp.where(mine, wide, 0.0).astype(BF)


def ffn_kernel(x_ref, wg_ref, wu_ref, wd_ref, out_ref, rows_ref, tail_ref):
    main = 8 * x_ref.shape[0]
    load_pairs(x_ref, rows_ref.at[pl.ds(main, rows_ref.shape[0] - main), :])
    for n in range(SUB // 2):
        rows_ref[:main, n * 256 : (n + 1) * 256] = columns_of(x_ref, n)
    x = rows_ref[...]
    gate = jnp.dot(x, wg_ref[...], preferred_element_type=F32)
    up = jnp.dot(x, wu_ref[...], preferred_element_type=F32)
    hidden = (gate / (1.0 + jnp.exp(-gate)) * up).astype(BF)
    for n in range(SUB // 2):
        cols = slice(n * 256, (n + 1) * 256)
        store_columns(jnp.dot(hidden, wd_ref[:, cols], preferred_element_type=F32).astype(BF), n, out_ref, tail_ref)
    store_pairs(tail_ref, out_ref)


def combine_kernel(mix_ref, x_ref, out_hbm, tail_ref, out_ref, sems):
    rows = out_ref.shape[0]
    main = 8 * x_ref.shape[0]
    load_pairs(x_ref, tail_ref)
    copies = []
    for n in range(SUB // 2):
        cols = slice(n * 256, (n + 1) * 256)
        mixed = jnp.dot(mix_ref[:, :main], columns_of(x_ref, n), preferred_element_type=F32)
        mixed += jnp.dot(mix_ref[:, main:], tail_ref[:, cols], preferred_element_type=F32)
        out_ref[:, cols] = (mixed[:rows] + mixed[rows:]).astype(BF)
        if n % 4 == 3:
            part = pl.ds((n // 4) * 1024, 1024)
            put = pltpu.make_async_copy(out_ref.at[:, part], out_hbm.at[:, part], sems.at[n // 4])
            put.start()
            copies.append(put)
    for put in copies:
        put.wait()


AXES = (("zh", 2), ("x", 4), ("zl", 2), ("y", 4), ("core", 2))
ORDER = ("zh", "zl", "core", "x", "y")


def group_position(expert):
    digit, rest = {}, expert
    for name, size in reversed(AXES):
        digit[name], rest = rest % size, rest // size
    place = jnp.zeros_like(expert)
    for name in ORDER:
        place = place * dict(AXES)[name] + digit[name]
    return place


def in_hbm(x):
    return pltpu.with_memory_space_constraint(x, pltpu.HBM)


def body(tokens, expert_ids, gate_probs, w_gate, w_up, w_down):
    rows, top = expert_ids.shape
    width = tokens.shape[1]
    experts = math.prod(size for _, size in AXES)
    slots = 5 * rows * top // (4 * experts)
    total = experts * slots
    vmem = pl.BlockSpec(memory_space=pltpu.VMEM)
    hbm = pl.BlockSpec(memory_space=pltpu.HBM)
    limit = pltpu.CompilerParams(vmem_limit_bytes=32 * 1024 * 1024)
    chunks = jax.ShapeDtypeStruct((experts, 2 * slots, 8, LANES), BF)
    tail = pltpu.VMEM((total - 8 * experts, width), BF)

    def exchange(x):
        wire = x.reshape(experts, slots * SUB, LANES)
        wire = lax.all_to_all(wire, ORDER, split_axis=0, concat_axis=0, tiled=True)
        return wire.reshape(chunks.shape)

    sent, mix = pl.pallas_call(
        functools.partial(dispatch_kernel, slots),
        out_shape=(chunks, jax.ShapeDtypeStruct((2 * rows, total), BF)),
        in_specs=[hbm, hbm, hbm],
        out_specs=(vmem, vmem),
        scratch_shapes=[
            pltpu.VMEM((top, rows), jnp.int32),
            pltpu.VMEM((top, rows), F32),
            pltpu.VMEM((rows, width), BF),
            tail,
            pltpu.SemaphoreType.DMA((3,)),
        ],
        compiler_params=limit,
        name="dispatch",
    )(in_hbm(expert_ids.T), in_hbm(gate_probs.T), in_hbm(tokens))

    made = pl.pallas_call(
        ffn_kernel,
        out_shape=chunks,
        in_specs=[vmem] * 4,
        out_specs=vmem,
        scratch_shapes=[pltpu.VMEM((total, width), BF), tail],
        compiler_params=limit,
        name="ffn",
    )(exchange(sent), w_gate[0], w_up[0], w_down[0])

    return pl.pallas_call(
        combine_kernel,
        out_shape=jax.ShapeDtypeStruct((rows, width), BF),
        in_specs=[vmem, vmem],
        out_specs=hbm,
        scratch_shapes=[tail, pltpu.VMEM((rows, width), BF), pltpu.SemaphoreType.DMA((2,))],
        compiler_params=limit,
        name="combine",
    )(mix, exchange(made))


def solution(mesh):
    names, sizes = zip(*AXES)
    fine = jax.sharding.Mesh(mesh.devices.reshape(sizes), names)
    return jax.shard_map(
        body,
        mesh=fine,
        in_specs=(P(names, None),) * 3 + (P(names, None, None),) * 3,
        out_specs=P(names, None),
        check_vma=False,
    )
```

```python
import functools
import math

import jax
import jax.numpy as jnp
from jax import lax
from jax.experimental import pallas as pl
from jax.experimental.pallas import tpu as pltpu
from jax.sharding import PartitionSpec as P

BF = jnp.bfloat16
F32 = jnp.float32
LANES = 128
SUB = 16


def pair_matrix(to_pairs):
    i = lax.broadcasted_iota(jnp.int32, (256, 256), 0)
    j = lax.broadcasted_iota(jnp.int32, (256, 256), 1)
    if to_pairs:
        source = (i // 2 % SUB) * 16 + (i // 32) * 2 + i % 2
    else:
        source = (i // 2 % 8) * 32 + (i // 16) * 2 + i % 2
    return (j == source).astype(F32).astype(BF)


def store_pairs(tail_ref, chunks):
    peers, tiles = chunks.shape[:2]
    pairs = pair_matrix(True)
    for b in range(peers // 16):
        halves = []
        for h in range(2):
            at = (2 * b + h) * SUB
            halves.append(
                jnp.concatenate(
                    [tail_ref[at : at + SUB, c * LANES : (c + 1) * LANES] for c in range(SUB)], axis=0
                )
            )
        moved = jnp.dot(pairs, jnp.concatenate(halves, axis=1), preferred_element_type=F32).astype(BF)
        for h in range(2):
            at = (2 * b + h) * 8
            chunks[at : at + 8, SUB:tiles] = moved[:, h * LANES : (h + 1) * LANES].reshape(8, tiles - SUB, 8, LANES)


def load_pairs(chunks, tail_ref):
    peers, tiles = chunks.shape[:2]
    pairs = pair_matrix(False)
    for b in range(peers // 16):
        halves = []
        for h in range(2):
            at = (2 * b + h) * 8
            halves.append(chunks[at : at + 8, SUB:tiles].reshape(256, LANES))
        moved = jnp.dot(pairs, jnp.concatenate(halves, axis=1), preferred_element_type=F32).astype(BF)
        for h in range(2):
            at = (2 * b + h) * SUB
            for c in range(SUB):
                tail_ref[at : at + SUB, c * LANES : (c + 1) * LANES] = moved[
                    c * SUB : (c + 1) * SUB, h * LANES : (h + 1) * LANES
                ]


def store_columns(result, n, chunks, tail_ref):
    peers = chunks.shape[0]
    main = 8 * peers
    for h in range(2):
        half = result[:, h * LANES : (h + 1) * LANES]
        chunks[:, 2 * n + h] = half[:main].reshape(peers, 8, LANES)
    tail_ref[:, n * 256 : (n + 1) * 256] = result[main:]


def columns_of(chunks, n):
    main = 8 * chunks.shape[0]
    return jnp.concatenate([chunks[:, 2 * n + h].reshape(main, LANES) for h in range(2)], axis=1)


def owner_and_slot(index, slots, experts):
    main = 8 * experts
    owner = jnp.where(index < main, index // 8, (index - main) // (slots - 8))
    slot = jnp.where(index < main, index % 8, 8 + (index - main) % (slots - 8))
    return owner, slot


def dispatch_kernel(slots, ids_hbm, prob_hbm, tok_hbm, out_ref, mix_ref, ids_ref, prob_ref, tok_ref, tail_ref, sems):
    top, rows = ids_ref.shape
    experts = out_ref.shape[0]
    total = experts * slots
    get_ids = pltpu.make_async_copy(ids_hbm, ids_ref, sems.at[0])
    get_prob = pltpu.make_async_copy(prob_hbm, prob_ref, sems.at[1])
    get_tok = pltpu.make_async_copy(tok_hbm, tok_ref, sems.at[2])
    get_ids.start()
    get_prob.start()
    get_tok.start()

    before = lax.broadcasted_iota(jnp.int32, (rows, rows), 0)
    after = lax.broadcasted_iota(jnp.int32, (rows, rows), 1)
    earlier = (before < after).astype(F32).astype(BF)
    owner, slot = owner_and_slot(lax.broadcasted_iota(jnp.int32, (total, experts), 0), slots, experts)
    from_expert = (owner == lax.broadcasted_iota(jnp.int32, (total, experts), 1)).astype(F32).astype(BF)
    get_ids.wait()
    get_prob.wait()
    place = group_position(ids_ref[...])
    prob = prob_ref[...]
    expert = lax.broadcasted_iota(jnp.int32, (experts, rows), 0)
    named = jnp.zeros((experts, rows), F32)
    weight = jnp.zeros((experts, rows), F32)
    for k in range(top):
        mine = place[k : k + 1, :] == expert
        named += mine.astype(F32)
        weight += jnp.where(mine, prob[k : k + 1, :], 0.0)
    rank = jnp.dot(named.astype(BF), earlier, preferred_element_type=F32)
    rank = jnp.where(named > 0.0, rank, -1.0)
    ranks = jnp.dot(from_expert, rank.astype(BF), preferred_element_type=F32)
    picked = (ranks == slot.astype(F32)).astype(F32).astype(BF)
    get_tok.wait()
    for n in range(SUB // 2):
        cols = slice(n * 256, (n + 1) * 256)
        store_columns(jnp.dot(picked, tok_ref[:, cols], preferred_element_type=F32).astype(BF), n, out_ref, tail_ref)
    store_pairs(tail_ref, out_ref)

    rank = rank.T.astype(BF)
    weight = weight.T
    high = weight.astype(BF)
    low = (weight - high.astype(F32)).astype(BF)
    owner, _ = owner_and_slot(lax.broadcasted_iota(jnp.int32, (experts, total), 1), slots, experts)
    _, slot = owner_and_slot(lax.broadcasted_iota(jnp.int32, (rows, total), 1), slots, experts)
    to_slot = (owner == lax.broadcasted_iota(jnp.int32, (experts, total), 0)).astype(F32).astype(BF)
    mine = jnp.dot(rank, to_slot, preferred_element_type=F32) == slot.astype(F32)
    for i, part in enumerate((high, low)):
        wide = jnp.dot(part, to_slot, preferred_element_type=F32)
        mix_ref[i * rows : (i + 1) * rows, :] = jnp.where(mine, wide, 0.0).astype(BF)


def ffn_kernel(x_ref, wg_ref, wu_ref, wd_ref, out_ref, rows_ref, tail_ref):
    main = 8 * x_ref.shape[0]
    load_pairs(x_ref, rows_ref.at[pl.ds(main, rows_ref.shape[0] - main), :])
    for n in range(SUB // 2):
        rows_ref[:main, n * 256 : (n + 1) * 256] = columns_of(x_ref, n)
    x = rows_ref[...]
    parts = []
    for j in range(wg_ref.shape[1] // 256):
        cols = slice(j * 256, (j + 1) * 256)
        gate = jnp.dot(x, wg_ref[:, cols], preferred_element_type=F32)
        up = jnp.dot(x, wu_ref[:, cols], preferred_element_type=F32)
        parts.append((gate / (1.0 + jnp.exp(-gate)) * up).astype(BF))
    hidden = jnp.concatenate(parts, axis=1)
    for n in range(SUB // 2):
        cols = slice(n * 256, (n + 1) * 256)
        store_columns(jnp.dot(hidden, wd_ref[:, cols], preferred_element_type=F32).astype(BF), n, out_ref, tail_ref)
    store_pairs(tail_ref, out_ref)


def combine_kernel(mix_ref, x_ref, out_hbm, tail_ref, out_ref, sems):
    rows = out_ref.shape[0]
    main = 8 * x_ref.shape[0]
    load_pairs(x_ref, tail_ref)
    copies = []
    for n in range(SUB // 2):
        cols = slice(n * 256, (n + 1) * 256)
        mixed = jnp.dot(mix_ref[:, :main], columns_of(x_ref, n), preferred_element_type=F32)
        mixed += jnp.dot(mix_ref[:, main:], tail_ref[:, cols], preferred_element_type=F32)
        out_ref[:, cols] = (mixed[:rows] + mixed[rows:]).astype(BF)
        if n % 4 == 3:
            part = pl.ds((n // 4) * 1024, 1024)
            put = pltpu.make_async_copy(out_ref.at[:, part], out_hbm.at[:, part], sems.at[n // 4])
            put.start()
            copies.append(put)
    for put in copies:
        put.wait()


AXES = (("zh", 2), ("x", 4), ("zl", 2), ("y", 4), ("core", 2))
ORDER = ("zl", "y", "core", "x", "zh")


def group_position(expert):
    digit, rest = {}, expert
    for name, size in reversed(AXES):
        digit[name], rest = rest % size, rest // size
    place = jnp.zeros_like(expert)
    for name in ORDER:
        place = place * dict(AXES)[name] + digit[name]
    return place


def in_hbm(x):
    return pltpu.with_memory_space_constraint(x, pltpu.HBM)


def body(tokens, expert_ids, gate_probs, w_gate, w_up, w_down):
    rows, top = expert_ids.shape
    width = tokens.shape[1]
    experts = math.prod(size for _, size in AXES)
    slots = 5 * rows * top // (4 * experts)
    total = experts * slots
    vmem = pl.BlockSpec(memory_space=pltpu.VMEM)
    hbm = pl.BlockSpec(memory_space=pltpu.HBM)
    limit = pltpu.CompilerParams(vmem_limit_bytes=32 * 1024 * 1024)
    chunks = jax.ShapeDtypeStruct((experts, 2 * slots, 8, LANES), BF)
    tail = pltpu.VMEM((total - 8 * experts, width), BF)

    def exchange(x):
        wire = x.reshape(experts, slots * SUB, LANES)
        wire = lax.all_to_all(wire, ORDER, split_axis=0, concat_axis=0, tiled=True)
        return wire.reshape(chunks.shape)

    sent, mix = pl.pallas_call(
        functools.partial(dispatch_kernel, slots),
        out_shape=(chunks, jax.ShapeDtypeStruct((2 * rows, total), BF)),
        in_specs=[hbm, hbm, hbm],
        out_specs=(vmem, vmem),
        scratch_shapes=[
            pltpu.VMEM((top, rows), jnp.int32),
            pltpu.VMEM((top, rows), F32),
            pltpu.VMEM((rows, width), BF),
            tail,
            pltpu.SemaphoreType.DMA((3,)),
        ],
        compiler_params=limit,
        name="dispatch",
    )(in_hbm(expert_ids.T), in_hbm(gate_probs.T), in_hbm(tokens))

    made = pl.pallas_call(
        ffn_kernel,
        out_shape=chunks,
        in_specs=[vmem] * 4,
        out_specs=vmem,
        scratch_shapes=[pltpu.VMEM((total, width), BF), tail],
        compiler_params=limit,
        name="ffn",
    )(exchange(sent), w_gate[0], w_up[0], w_down[0])

    return pl.pallas_call(
        combine_kernel,
        out_shape=jax.ShapeDtypeStruct((rows, width), BF),
        in_specs=[vmem, vmem],
        out_specs=hbm,
        scratch_shapes=[tail, pltpu.VMEM((rows, width), BF), pltpu.SemaphoreType.DMA((2,))],
        compiler_params=limit,
        name="combine",
    )(mix, exchange(made))


def solution(mesh):
    names, sizes = zip(*AXES)
    fine = jax.sharding.Mesh(mesh.devices.reshape(sizes), names)
    return jax.shard_map(
        body,
        mesh=fine,
        in_specs=(P(names, None),) * 3 + (P(names, None, None),) * 3,
        out_specs=P(names, None),
        check_vma=False,
    )
```

```python
import functools
import math

import jax
import jax.numpy as jnp
from jax import lax
from jax.experimental import pallas as pl
from jax.experimental.pallas import tpu as pltpu
from jax.sharding import PartitionSpec as P

BF = jnp.bfloat16
F32 = jnp.float32
LANES = 128
SUB = 16


def pair_matrix(to_pairs):
    i = lax.broadcasted_iota(jnp.int32, (256, 256), 0)
    j = lax.broadcasted_iota(jnp.int32, (256, 256), 1)
    if to_pairs:
        source = (i // 2 % SUB) * 16 + (i // 32) * 2 + i % 2
    else:
        source = (i // 2 % 8) * 32 + (i // 16) * 2 + i % 2
    return (j == source).astype(F32).astype(BF)


def store_pairs(tail_ref, chunks):
    peers, tiles = chunks.shape[:2]
    pairs = pair_matrix(True)
    for b in range(peers // 16):
        halves = []
        for h in range(2):
            at = (2 * b + h) * SUB
            halves.append(
                jnp.concatenate(
                    [tail_ref[at : at + SUB, c * LANES : (c + 1) * LANES] for c in range(SUB)], axis=0
                )
            )
        moved = jnp.dot(pairs, jnp.concatenate(halves, axis=1), preferred_element_type=F32).astype(BF)
        for h in range(2):
            at = (2 * b + h) * 8
            chunks[at : at + 8, SUB:tiles] = moved[:, h * LANES : (h + 1) * LANES].reshape(8, tiles - SUB, 8, LANES)


def load_pairs(chunks, tail_ref):
    peers, tiles = chunks.shape[:2]
    pairs = pair_matrix(False)
    for b in range(peers // 16):
        halves = []
        for h in range(2):
            at = (2 * b + h) * 8
            halves.append(chunks[at : at + 8, SUB:tiles].reshape(256, LANES))
        moved = jnp.dot(pairs, jnp.concatenate(halves, axis=1), preferred_element_type=F32).astype(BF)
        for h in range(2):
            at = (2 * b + h) * SUB
            for c in range(SUB):
                tail_ref[at : at + SUB, c * LANES : (c + 1) * LANES] = moved[
                    c * SUB : (c + 1) * SUB, h * LANES : (h + 1) * LANES
                ]


def store_columns(result, n, chunks, tail_ref):
    peers = chunks.shape[0]
    main = 8 * peers
    for h in range(2):
        half = result[:, h * LANES : (h + 1) * LANES]
        chunks[:, 2 * n + h] = half[:main].reshape(peers, 8, LANES)
    tail_ref[:, n * 256 : (n + 1) * 256] = result[main:]


def columns_of(chunks, n):
    main = 8 * chunks.shape[0]
    return jnp.concatenate([chunks[:, 2 * n + h].reshape(main, LANES) for h in range(2)], axis=1)


def owner_and_slot(index, slots, experts):
    main = 8 * experts
    owner = jnp.where(index < main, index // 8, (index - main) // (slots - 8))
    slot = jnp.where(index < main, index % 8, 8 + (index - main) % (slots - 8))
    return owner, slot


def dispatch_kernel(slots, ids_hbm, prob_hbm, tok_hbm, out_ref, mix_ref, ids_ref, prob_ref, tok_ref, tail_ref, sems):
    top, rows = ids_ref.shape
    experts = out_ref.shape[0]
    total = experts * slots
    get_ids = pltpu.make_async_copy(ids_hbm, ids_ref, sems.at[0])
    get_prob = pltpu.make_async_copy(prob_hbm, prob_ref, sems.at[1])
    get_tok = pltpu.make_async_copy(tok_hbm, tok_ref, sems.at[2])
    get_ids.start()
    get_prob.start()
    get_tok.start()

    before = lax.broadcasted_iota(jnp.int32, (rows, rows), 0)
    after = lax.broadcasted_iota(jnp.int32, (rows, rows), 1)
    earlier = (before < after).astype(F32).astype(BF)
    owner, slot = owner_and_slot(lax.broadcasted_iota(jnp.int32, (total, experts), 0), slots, experts)
    from_expert = (owner == lax.broadcasted_iota(jnp.int32, (total, experts), 1)).astype(F32).astype(BF)
    get_ids.wait()
    get_prob.wait()
    place = group_position(ids_ref[...])
    prob = prob_ref[...]
    expert = lax.broadcasted_iota(jnp.int32, (experts, rows), 0)
    named = jnp.zeros((experts, rows), F32)
    weight = jnp.zeros((experts, rows), F32)
    for k in range(top):
        mine = place[k : k + 1, :] == expert
        named += mine.astype(F32)
        weight += jnp.where(mine, prob[k : k + 1, :], 0.0)
    rank = jnp.dot(named.astype(BF), earlier, preferred_element_type=F32)
    rank = jnp.where(named > 0.0, rank, -1.0)
    ranks = jnp.dot(from_expert, rank.astype(BF), preferred_element_type=F32)
    picked = (ranks == slot.astype(F32)).astype(F32).astype(BF)
    get_tok.wait()
    for n in range(SUB // 2):
        cols = slice(n * 256, (n + 1) * 256)
        store_columns(jnp.dot(picked, tok_ref[:, cols], preferred_element_type=F32).astype(BF), n, out_ref, tail_ref)
    store_pairs(tail_ref, out_ref)

    rank = rank.T.astype(BF)
    weight = weight.T
    high = weight.astype(BF)
    low = (weight - high.astype(F32)).astype(BF)
    owner, _ = owner_and_slot(lax.broadcasted_iota(jnp.int32, (experts, total), 1), slots, experts)
    _, slot = owner_and_slot(lax.broadcasted_iota(jnp.int32, (rows, total), 1), slots, experts)
    to_slot = (owner == lax.broadcasted_iota(jnp.int32, (experts, total), 0)).astype(F32).astype(BF)
    mine = jnp.dot(rank, to_slot, preferred_element_type=F32) == slot.astype(F32)
    for i, part in enumerate((high, low)):
        wide = jnp.dot(part, to_slot, preferred_element_type=F32)
        mix_ref[i * rows : (i + 1) * rows, :] = jnp.where(mine, wide, 0.0).astype(BF)


def ffn_kernel(x_ref, wg_ref, wu_ref, wd_ref, out_ref, rows_ref, tail_ref):
    main = 8 * x_ref.shape[0]
    load_pairs(x_ref, rows_ref.at[pl.ds(main, rows_ref.shape[0] - main), :])
    for n in range(SUB // 2):
        rows_ref[:main, n * 256 : (n + 1) * 256] = columns_of(x_ref, n)
    x = rows_ref[...]
    parts = []
    for j in range(wg_ref.shape[1] // 256):
        cols = slice(j * 256, (j + 1) * 256)
        gate = jnp.dot(x, wg_ref[:, cols], preferred_element_type=F32)
        up = jnp.dot(x, wu_ref[:, cols], preferred_element_type=F32)
        parts.append((gate / (1.0 + jnp.exp(-gate)) * up).astype(BF))
    hidden = jnp.concatenate(parts, axis=1)
    for n in range(SUB // 2):
        cols = slice(n * 256, (n + 1) * 256)
        tail_ref[:, cols] = jnp.dot(hidden[main:], wd_ref[:, cols], preferred_element_type=F32).astype(BF)
    store_pairs(tail_ref, out_ref)
    for n in range(SUB // 2):
        cols = slice(n * 256, (n + 1) * 256)
        result = jnp.dot(hidden[:main], wd_ref[:, cols], preferred_element_type=F32).astype(BF)
        for h in range(2):
            out_ref[:, 2 * n + h] = result[:, h * LANES : (h + 1) * LANES].reshape(main // 8, 8, LANES)


def combine_kernel(mix_ref, x_ref, out_hbm, tail_ref, out_ref, sems):
    rows = out_ref.shape[0]
    main = 8 * x_ref.shape[0]
    load_pairs(x_ref, tail_ref)
    copies = []
    for n in range(SUB // 2):
        cols = slice(n * 256, (n + 1) * 256)
        mixed = jnp.dot(mix_ref[:, :main], columns_of(x_ref, n), preferred_element_type=F32)
        mixed += jnp.dot(mix_ref[:, main:], tail_ref[:, cols], preferred_element_type=F32)
        out_ref[:, cols] = (mixed[:rows] + mixed[rows:]).astype(BF)
        if n % 4 == 3:
            part = pl.ds((n // 4) * 1024, 1024)
            put = pltpu.make_async_copy(out_ref.at[:, part], out_hbm.at[:, part], sems.at[n // 4])
            put.start()
            copies.append(put)
    for put in copies:
        put.wait()


AXES = (("zh", 2), ("x", 4), ("zl", 2), ("y", 4), ("core", 2))
ORDER = ("zl", "y", "core", "x", "zh")


def group_position(expert):
    digit, rest = {}, expert
    for name, size in reversed(AXES):
        digit[name], rest = rest % size, rest // size
    place = jnp.zeros_like(expert)
    for name in ORDER:
        place = place * dict(AXES)[name] + digit[name]
    return place


def in_hbm(x):
    return pltpu.with_memory_space_constraint(x, pltpu.HBM)


def body(tokens, expert_ids, gate_probs, w_gate, w_up, w_down):
    rows, top = expert_ids.shape
    width = tokens.shape[1]
    experts = math.prod(size for _, size in AXES)
    slots = 5 * rows * top // (4 * experts)
    total = experts * slots
    vmem = pl.BlockSpec(memory_space=pltpu.VMEM)
    hbm = pl.BlockSpec(memory_space=pltpu.HBM)
    limit = pltpu.CompilerParams(vmem_limit_bytes=32 * 1024 * 1024)
    chunks = jax.ShapeDtypeStruct((experts, 2 * slots, 8, LANES), BF)
    tail = pltpu.VMEM((total - 8 * experts, width), BF)

    def exchange(x):
        wire = x.reshape(experts, slots * SUB, LANES)
        wire = lax.all_to_all(wire, ORDER, split_axis=0, concat_axis=0, tiled=True)
        return wire.reshape(chunks.shape)

    sent, mix = pl.pallas_call(
        functools.partial(dispatch_kernel, slots),
        out_shape=(chunks, jax.ShapeDtypeStruct((2 * rows, total), BF)),
        in_specs=[hbm, hbm, hbm],
        out_specs=(vmem, vmem),
        scratch_shapes=[
            pltpu.VMEM((top, rows), jnp.int32),
            pltpu.VMEM((top, rows), F32),
            pltpu.VMEM((rows, width), BF),
            tail,
            pltpu.SemaphoreType.DMA((3,)),
        ],
        compiler_params=limit,
        name="dispatch",
    )(in_hbm(expert_ids.T), in_hbm(gate_probs.T), in_hbm(tokens))

    made = pl.pallas_call(
        ffn_kernel,
        out_shape=chunks,
        in_specs=[vmem] * 4,
        out_specs=vmem,
        scratch_shapes=[pltpu.VMEM((total, width), BF), tail],
        compiler_params=limit,
        name="ffn",
    )(exchange(sent), w_gate[0], w_up[0], w_down[0])

    return pl.pallas_call(
        combine_kernel,
        out_shape=jax.ShapeDtypeStruct((rows, width), BF),
        in_specs=[vmem, vmem],
        out_specs=hbm,
        scratch_shapes=[tail, pltpu.VMEM((rows, width), BF), pltpu.SemaphoreType.DMA((2,))],
        compiler_params=limit,
        name="combine",
    )(mix, exchange(made))


def solution(mesh):
    names, sizes = zip(*AXES)
    fine = jax.sharding.Mesh(mesh.devices.reshape(sizes), names)
    return jax.shard_map(
        body,
        mesh=fine,
        in_specs=(P(names, None),) * 3 + (P(names, None, None),) * 3,
        out_specs=P(names, None),
        check_vma=False,
    )
```
